32 devices in a mesh: elem: 16 (over z, y, core), test: 2 (over x).
Axes of the slice: x: 2, y: 2, z: 4, core: 2. Of those that a mesh axis runs over, the one named last changes fastest.
Arguments:
- mode_fields: bfloat16 [64, 3, 65536], P('test', None, 'elem'), may hold values from -6 to 6
- elem_type: int32 [128], P('elem'), may hold values from 0 to 3
- type_scales: float32 [4, 3], replicated, may hold values from 0.5 to 2
Outputs:
- conv_tensor: float32 [64, 64, 64], P('test', 'elem')
The draws below stay inside these ranges and needn't reach their ends.
All inputs are finite; a program needn't handle non-finite values.
Results may differ from the reference program's by a relative error of at most 0.0051.
Values may be sent and summed in bfloat16 or wider, within the bound.
A program may use at most 64 MiB of HBM per device.

```python
import math
import jax
import jax.numpy as jnp
import numpy as np
from jax import lax

M = 64
Q = 8
TYPES = 4
NELEM = 128
NPTS = 65536
N_ELEM = 16
N_TEST = 2


def set_ends(values, key, low, top_value):
    place = [jax.random.randint(jax.random.fold_in(key, axis), (), 0, length) for axis, length in enumerate(values.shape)]
    widest = values.shape.index(max(values.shape))
    beside = place[:widest] + [(place[widest] + 1) % values.shape[widest]] + place[widest + 1:]
    return values.at[tuple(place)].set(low).at[tuple(beside)].set(top_value)


def block_scale(key, dims, split, smallest, high):
    factor_of = 1.0
    for axis_at, blocks in split:
        heights = jax.random.uniform(jax.random.fold_in(jax.random.fold_in(key, 6), axis_at), (blocks,), jnp.float32, smallest / len(split), high / len(split))
        factor_of = factor_of * jnp.repeat(jnp.exp(heights), dims[axis_at] // blocks).reshape((-1,) + (1,) * (len(dims) - 1 - axis_at))
    return factor_of


def bell_draw(own_key, shape, spread, most, split=(), held_as=jnp.bfloat16):
    factor_of = block_scale(own_key, shape, split, -0.22, 0.18) if split else 1.0
    values = jax.random.normal(own_key, shape, jnp.float32) * spread * factor_of
    return jnp.minimum(jnp.maximum(values, -most), most).astype(held_as)


def setup_inputs(seed: int = 0) -> dict:
    streams_of = jax.random.split(jax.random.key(seed), 4)
    return {
        "mode_fields": bell_draw(streams_of[0], (M, 3, NPTS), 1.0, 6.0, ((0, 2), (2, 16))),
        "elem_type": set_ends(jax.random.randint(streams_of[1], (NELEM,), 0, TYPES), jax.random.fold_in(streams_of[1], 1), 0, TYPES - 1).astype(jnp.int32),
        "type_scales": jnp.clip(jnp.exp(jax.random.uniform(streams_of[2], (TYPES, 3), jnp.float32, math.log(0.5), math.log(2.0))), 0.5, 2.0),
    }


block_modes = 4


def legendre_top(points, degree):
    before = points * 0.0 + 1.0
    current = points
    for order in range(2, degree + 1):
        following = ((2 * order - 1) * points * current - (order - 1) * before) / order
        before = current
        current = following
    return current, before


def lobatto_tables(order_points):
    degree = order_points - 1
    lobatto_nodes = np.cos(np.pi * np.arange(degree + 1) / degree)
    for sweep in range(100):
        top, lower = legendre_top(lobatto_nodes, degree)
        lobatto_nodes = lobatto_nodes - (lobatto_nodes * top - lower) / ((degree + 1) * top)
    lobatto_nodes = lobatto_nodes[::-1].copy()
    lobatto_nodes[0] = -1.0
    lobatto_nodes[-1] = 1.0
    values, unused = legendre_top(lobatto_nodes, degree)
    weights = 2.0 / (degree * (degree + 1) * values ** 2)
    identity = np.eye(order_points)
    distance = lobatto_nodes[:, None] - lobatto_nodes[None, :]
    spacing = np.where(identity > 0, 1.0, distance)
    derivative = np.where(identity > 0, 0.0, values[:, None] / values[None, :] / spacing)
    corner = degree * (degree + 1) / 4.0
    ends = np.concatenate([[-corner], np.zeros(degree - 1), [corner]])
    derivative = derivative + identity * ends[None, :]
    square_eye = np.eye(order_points * order_points)
    along_r = np.kron(square_eye, derivative)
    along_s = np.kron(identity, np.kron(derivative, identity))
    along_t = np.kron(derivative, square_eye)
    table = np.concatenate([along_r.T, along_s.T, along_t.T], axis=1)
    cube_weights = np.kron(weights, np.kron(weights, weights))
    return table.astype(np.float32), cube_weights.astype(np.float32)


def element_scales(types, type_scales):
    picks = (types[:, None] == jnp.arange(type_scales.shape[0], dtype=jnp.int32)[None, :]).astype(jnp.float32)
    return jnp.sum(picks[:, :, None] * type_scales[None, :, :], axis=1)


def gradient(fields, scales, table, cube):
    mode_count = fields.shape[0]
    elements = fields.shape[2] // cube
    flat = fields.reshape(mode_count * 3 * elements, cube)
    derived = jnp.dot(flat, table, preferred_element_type=jnp.float32).reshape(mode_count, 3, elements, 3, cube)
    return (derived * scales[None, None, :, :, None]).astype(jnp.bfloat16)


def project(test_fields, trial_fields, grads, quadrature):
    test_modes = test_fields.shape[0]
    trial_modes = trial_fields.shape[0]
    grad_modes = grads.shape[0]
    blocks = grads.reshape((grad_modes // block_modes, block_modes) + grads.shape[1:])
    test_wide = test_fields.astype(jnp.float32)
    trial_wide = trial_fields.astype(jnp.float32)

    def one_block(grad_block):
        grad_wide = grad_block.astype(jnp.float32)
        summed = test_wide[:, None, 0, :, None, :] * grad_wide[None, :, 0]
        summed = summed + test_wide[:, None, 1, :, None, :] * grad_wide[None, :, 1]
        summed = summed + test_wide[:, None, 2, :, None, :] * grad_wide[None, :, 2]
        pairs = (summed * quadrature[None, None, :, None, :]).astype(jnp.bfloat16)
        return jnp.einsum('ikedp,jdep->ijk', pairs.astype(jnp.float32), trial_wide)

    result = lax.map(one_block, blocks)
    return result.transpose(1, 2, 0, 3).reshape(test_modes, trial_modes, grad_modes)


def reference(mode_fields, elem_type, type_scales):
    table, cube_weights = lobatto_tables(Q)
    table = jnp.asarray(table).astype(jnp.bfloat16)
    point_weights = jnp.asarray(cube_weights).astype(jnp.float32)
    cube = Q ** 3
    nblocks = N_ELEM * N_TEST
    per_block = NELEM // nblocks

    def step(total, inputs):
        index, types_block = inputs
        start = (index * (per_block * cube)).astype(jnp.int32)
        block = lax.dynamic_slice_in_dim(mode_fields, start, per_block * cube, 2)
        scales = element_scales(types_block, type_scales)
        quadrature = point_weights[None, :] / jnp.prod(scales, axis=1)[:, None]
        grads = gradient(block, scales, table, cube)
        shaped = block.reshape(M, 3, per_block, cube)
        return total + project(shaped, shaped, grads, quadrature), None

    total, _ = lax.scan(step, jnp.zeros((M, M, M), jnp.float32),
                        (jnp.arange(nblocks, dtype=jnp.int32), elem_type.reshape(nblocks, per_block)))
    return total * (float(NPTS) ** -0.5)
```

```python
import jax
import jax.numpy as jnp
import numpy as np
from jax import lax
from jax.experimental import pallas as pl
from jax.experimental.pallas import tpu as pltpu
from jax.sharding import PartitionSpec as P

Q = 8


block_modes = 8
rows16 = 16


def legendre_top(points, degree):
    before = points * 0.0 + 1.0
    current = points
    for order in range(2, degree + 1):
        following = ((2 * order - 1) * points * current - (order - 1) * before) / order
        before = current
        current = following
    return (current, before)


def lobatto_tables(order_points):
    degree = order_points - 1
    lobatto_nodes = np.cos(np.pi * np.arange(degree + 1) / degree)
    for sweep in range(100):
        top, lower = legendre_top(lobatto_nodes, degree)
        lobatto_nodes = lobatto_nodes - (lobatto_nodes * top - lower) / ((degree + 1) * top)
    lobatto_nodes = lobatto_nodes[::-1].copy()
    lobatto_nodes[0] = -1.0
    lobatto_nodes[-1] = 1.0
    values, unused = legendre_top(lobatto_nodes, degree)
    weights = 2.0 / (degree * (degree + 1) * values**2)
    identity = np.eye(order_points)
    distance = lobatto_nodes[:, None] - lobatto_nodes[None, :]
    spacing = np.where(identity > 0, 1.0, distance)
    derivative = np.where(identity > 0, 0.0, values[:, None] / values[None, :] / spacing)
    corner = degree * (degree + 1) / 4.0
    ends = np.concatenate([[-corner], np.zeros(degree - 1), [corner]])
    derivative = derivative + identity * ends[None, :]
    square_eye = np.eye(order_points * order_points)
    along_r = np.kron(square_eye, derivative)
    along_s = np.kron(identity, np.kron(derivative, identity))
    along_t = np.kron(derivative, square_eye)
    table = np.concatenate([along_r.T, along_s.T, along_t.T], axis=1)
    cube_weights = np.kron(weights, np.kron(weights, weights))
    return (table.astype(np.float32), cube_weights.astype(np.float32))


def kernel(
    n_test, n_elem, final_scale,
    x_ref, types, type_scales, table_rs, table_t, weights,
    out_ref,
    fields, grads, wide, rhs, totals, outgoing, incoming,
    local_sem, send_sem, recv_sem, send_sum, recv_sum,
):
    elements, _, modes, cube = x_ref.shape
    all_modes = n_test * modes
    half = cube // 2
    owned = all_modes // n_elem
    blocks = modes // block_modes
    t = lax.axis_index("test")
    me = lax.axis_index("elem")

    def local_copy(e):
        return pltpu.make_async_copy(x_ref.at[e], fields.at[t, e], local_sem.at[e])

    def panel_copy(off, e):
        return pltpu.make_async_remote_copy(
            src_ref=fields.at[t, e],
            dst_ref=fields.at[t, e],
            send_sem=send_sem.at[off - 1, e],
            recv_sem=recv_sem.at[off - 1, e],
            device_id={"test": lax.rem(t + off, n_test)},
            device_id_type=pl.DeviceIdType.MESH,
        )

    def sum_copy(off):
        return pltpu.make_async_remote_copy(
            src_ref=outgoing.at[lax.rem(me + off, n_elem)],
            dst_ref=incoming.at[off - 1],
            send_sem=send_sum.at[off - 1],
            recv_sem=recv_sum.at[off - 1],
            device_id={"elem": lax.rem(me + off, n_elem)},
            device_id_type=pl.DeviceIdType.MESH,
        )

    for e in range(elements):
        local_copy(e).start()

    barrier = pltpu.get_barrier_semaphore()
    for off in range(1, n_test):
        pl.semaphore_signal(
            barrier, inc=1, device_id={"test": lax.rem(t + off, n_test)},
            device_id_type=pl.DeviceIdType.MESH,
        )
    for off in range(1, n_elem):
        pl.semaphore_signal(
            barrier, inc=1, device_id={"elem": lax.rem(me + off, n_elem)},
            device_id_type=pl.DeviceIdType.MESH,
        )
    pl.semaphore_wait(barrier, n_test + n_elem - 2)

    for e in range(elements):
        local_copy(e).wait()
        for off in range(1, n_test):
            panel_copy(off, e).start()

    totals[...] = jnp.zeros_like(totals)

    def element(e, carry):
        for off in range(1, n_test):
            panel_copy(off, e).wait_recv()
        kind = types[e]
        scale = [type_scales[kind, d] for d in range(3)]
        volume = jnp.full((1, cube), scale[0] * scale[1] * scale[2], jnp.float32)
        quadrature = weights[...] / volume
        factor = [quadrature * scale[d] for d in range(3)]
        held = [
            jnp.concatenate([fields[n, e, c] for n in range(n_test)], axis=0) for c in range(3)
        ]
        stacked = jnp.concatenate(held, axis=0)
        for h in range(2):
            part = slice(h * half, (h + 1) * half)
            derived = jnp.dot(
                stacked[:, part], table_rs[...], preferred_element_type=jnp.float32
            )
            for d in range(2):
                grads[d, :, part] = (
                    derived[:, d * half : (d + 1) * half] * factor[d][:, part]
                ).astype(jnp.bfloat16)
        derived = jnp.dot(stacked, table_t[...], preferred_element_type=jnp.float32)
        grads[2] = (derived * factor[2]).astype(jnp.bfloat16)
        for d in range(3):
            rhs[d] = held[d].T
        for c in range(3):
            own = fields[t, e, c].astype(jnp.float32)
            for i in range(modes):
                wide[c * modes + i] = jnp.broadcast_to(own[i : i + 1], (rows16, cube)).astype(
                    jnp.bfloat16
                )

        def block(ib, inner):
            total = jnp.zeros((block_modes * all_modes, all_modes), jnp.float32)
            for d in range(3):
                for h in range(2):
                    part = slice(h * half, (h + 1) * half)
                    g = [
                        grads[d, c * all_modes : (c + 1) * all_modes, part].reshape(
                            all_modes // rows16, rows16, half
                        )
                        for c in range(3)
                    ]
                    pairs = []
                    for i in range(block_modes):
                        row = ib * block_modes + i
                        f = [wide[c * modes + row, :, part][None] for c in range(3)]
                        summed = f[0] * g[0] + f[1] * g[1] + f[2] * g[2]
                        pairs.append(summed.reshape(all_modes, half))
                    total = total + jnp.dot(
                        jnp.concatenate(pairs, axis=0),
                        rhs[d, part, :],
                        preferred_element_type=jnp.float32,
                    )
            totals[ib] += total
            return inner

        return lax.fori_loop(0, blocks, block, carry)

    lax.fori_loop(0, elements, element, 0)

    turned = [totals[ib].T for ib in range(blocks)]
    for b in range(n_elem):
        outgoing[b] = jnp.concatenate(
            [turned[ib][b * owned : (b + 1) * owned] for ib in range(blocks)], axis=0
        ).astype(jnp.bfloat16)
    for off in range(1, n_elem):
        sum_copy(off).start()
    result = outgoing[me].astype(jnp.float32)
    for off in range(1, n_elem):
        sum_copy(off).wait_recv()
        result = result + incoming[off - 1].astype(jnp.float32)
    out_ref[...] = result * final_scale

    for off in range(1, n_elem):
        sum_copy(off).wait_send()

    def drain(e, carry):
        for off in range(1, n_test):
            panel_copy(off, e).wait_send()
        return carry

    lax.fori_loop(0, elements, drain, 0)


def split_tables(order_points):
    table, cube_weights = lobatto_tables(order_points)
    cube = order_points**3
    half = cube // 2
    table_rs = np.concatenate([table[:half, :half], table[:half, cube : cube + half]], axis=1)
    table_t = table[:, 2 * cube :]
    return table_rs, table_t, cube_weights


def body(mode_fields, elem_type, type_scales):
    n_test = lax.axis_size("test")
    n_elem = lax.axis_size("elem")
    cube = Q**3
    modes, _, points = mode_fields.shape
    elements = points // cube
    all_modes = modes * n_test
    owned = all_modes // n_elem
    blocks = modes // block_modes
    table_rs, table_t, cube_weights = split_tables(Q)
    chunks = mode_fields.reshape(modes, 3, elements, cube).transpose(2, 1, 0, 3)
    final_scale = float(points * n_elem) ** (-0.5)
    rows = blocks * owned
    lanes = block_modes * all_modes
    vmem = pl.BlockSpec(memory_space=pltpu.VMEM)
    smem = pl.BlockSpec(memory_space=pltpu.SMEM)

    def call(*args):
        kernel(n_test, n_elem, final_scale, *args)

    out = pl.pallas_call(
        call,
        out_shape=jax.ShapeDtypeStruct((rows, lanes), jnp.float32),
        in_specs=[pl.BlockSpec(memory_space=pl.ANY), smem, smem, vmem, vmem, vmem],
        out_specs=vmem,
        scratch_shapes=[
            pltpu.VMEM((n_test, elements, 3, modes, cube), jnp.bfloat16),
            pltpu.VMEM((3, 3 * all_modes, cube), jnp.bfloat16),
            pltpu.VMEM((3 * modes, rows16, cube), jnp.bfloat16),
            pltpu.VMEM((3, cube, all_modes), jnp.bfloat16),
            pltpu.VMEM((blocks, lanes, all_modes), jnp.float32),
            pltpu.VMEM((n_elem, rows, lanes), jnp.bfloat16),
            pltpu.VMEM((n_elem - 1, rows, lanes), jnp.bfloat16),
            pltpu.SemaphoreType.DMA((elements,)),
            pltpu.SemaphoreType.DMA((n_test - 1, elements)),
            pltpu.SemaphoreType.DMA((n_test - 1, elements)),
            pltpu.SemaphoreType.DMA((n_elem - 1,)),
            pltpu.SemaphoreType.DMA((n_elem - 1,)),
        ],
        compiler_params=pltpu.CompilerParams(
            collective_id=0, has_side_effects=True, vmem_limit_bytes=48 * 2**20
        ),
    )(
        chunks,
        elem_type,
        type_scales,
        jnp.asarray(table_rs).astype(jnp.bfloat16),
        jnp.asarray(table_t).astype(jnp.bfloat16),
        jnp.asarray(cube_weights)[None, :],
    )
    return (
        out.reshape(blocks, owned, block_modes, all_modes)
        .transpose(0, 2, 1, 3)
        .reshape(modes, owned, all_modes)
    )


def solution(mesh):
    placed = (P("test", None, "elem"), P("elem"), P())
    return jax.shard_map(
        body, mesh=mesh, in_specs=placed, out_specs=P("test", "elem", None), check_vma=False
    )
```

```python
import jax
import jax.numpy as jnp
import numpy as np
from jax import lax
from jax.experimental import pallas as pl
from jax.experimental.pallas import tpu as pltpu
from jax.sharding import PartitionSpec as P

Q = 8


block_modes = 8
rows16 = 16
lane_width = 128
tail_elements = 2


def legendre_top(points, degree):
    before = points * 0.0 + 1.0
    current = points
    for order in range(2, degree + 1):
        following = ((2 * order - 1) * points * current - (order - 1) * before) / order
        before = current
        current = following
    return (current, before)


def lobatto_tables(order_points):
    degree = order_points - 1
    lobatto_nodes = np.cos(np.pi * np.arange(degree + 1) / degree)
    for sweep in range(100):
        top, lower = legendre_top(lobatto_nodes, degree)
        lobatto_nodes = lobatto_nodes - (lobatto_nodes * top - lower) / ((degree + 1) * top)
    lobatto_nodes = lobatto_nodes[::-1].copy()
    lobatto_nodes[0] = -1.0
    lobatto_nodes[-1] = 1.0
    values, unused = legendre_top(lobatto_nodes, degree)
    weights = 2.0 / (degree * (degree + 1) * values**2)
    identity = np.eye(order_points)
    distance = lobatto_nodes[:, None] - lobatto_nodes[None, :]
    spacing = np.where(identity > 0, 1.0, distance)
    derivative = np.where(identity > 0, 0.0, values[:, None] / values[None, :] / spacing)
    corner = degree * (degree + 1) / 4.0
    ends = np.concatenate([[-corner], np.zeros(degree - 1), [corner]])
    derivative = derivative + identity * ends[None, :]
    square_eye = np.eye(order_points * order_points)
    along_r = np.kron(square_eye, derivative)
    along_s = np.kron(identity, np.kron(derivative, identity))
    along_t = np.kron(derivative, square_eye)
    table = np.concatenate([along_r.T, along_s.T, along_t.T], axis=1)
    cube_weights = np.kron(weights, np.kron(weights, weights))
    return (table.astype(np.float32), cube_weights.astype(np.float32))


def kernel(
    n_test, n_elem, elements, final_scale,
    x_ref, types, type_scales, far_rs, far_t, weights,
    out_ref,
    table_rs, table_t, table_sem, fields, grads, wide, rhs, totals, outgoing, incoming,
    local_sem, send_sem, recv_sem, send_sum, recv_sum,
):
    _, modes, points = x_ref.shape
    cube = points // elements
    all_modes = n_test * modes
    half = cube // 2
    owned = all_modes // n_elem
    blocks = modes // block_modes
    parts = block_modes * all_modes // lane_width
    tail = min(tail_elements, elements)
    t = lax.axis_index("test")
    me = lax.axis_index("elem")

    def local_copy(e):
        return pltpu.make_async_copy(
            x_ref.at[:, :, pl.ds(e * cube, cube)], fields.at[t, e], local_sem.at[e]
        )

    def panel_copy(off, e):
        return pltpu.make_async_remote_copy(
            src_ref=fields.at[t, e],
            dst_ref=fields.at[t, e],
            send_sem=send_sem.at[off - 1, e],
            recv_sem=recv_sem.at[off - 1, e],
            device_id={"test": lax.rem(t + off, n_test)},
            device_id_type=pl.DeviceIdType.MESH,
        )

    def sum_copy(off, ib):
        return pltpu.make_async_remote_copy(
            src_ref=outgoing.at[ib, lax.rem(me + off, n_elem)],
            dst_ref=incoming.at[ib, off - 1],
            send_sem=send_sum.at[ib, off - 1],
            recv_sem=recv_sum.at[ib, off - 1],
            device_id={"elem": lax.rem(me + off, n_elem)},
            device_id_type=pl.DeviceIdType.MESH,
        )

    barrier = pltpu.get_barrier_semaphore()
    for off in range(1, n_test):
        pl.semaphore_signal(
            barrier, inc=1, device_id={"test": lax.rem(t + off, n_test)},
            device_id_type=pl.DeviceIdType.MESH,
        )
    for off in range(1, n_elem):
        pl.semaphore_signal(
            barrier, inc=1, device_id={"elem": lax.rem(me + off, n_elem)},
            device_id_type=pl.DeviceIdType.MESH,
        )
    for e in range(elements):
        local_copy(e).start()
    tables = [
        pltpu.make_async_copy(far_rs, table_rs, table_sem.at[0]),
        pltpu.make_async_copy(far_t, table_t, table_sem.at[1]),
    ]
    for copy in tables:
        copy.start()
    pl.semaphore_wait(barrier, n_test + n_elem - 2)

    for e in range(elements):
        local_copy(e).wait()
        for off in range(1, n_test):
            panel_copy(off, e).start()

    for copy in tables:
        copy.wait()

    def differentiate(n, e):
        kind = types[e]
        scale = [type_scales[kind, d] for d in range(3)]
        volume = jnp.full((1, cube), scale[0] * scale[1] * scale[2], jnp.float32)
        quadrature = weights[...] / volume
        factor = [quadrature * scale[d] for d in range(3)]
        stacked = jnp.concatenate([fields[n, e, c] for c in range(3)], axis=0)
        for h in range(2):
            part = slice(h * half, (h + 1) * half)
            derived = jnp.dot(
                stacked[:, part], table_rs[...], preferred_element_type=jnp.float32
            )
            for d in range(2):
                value = derived[:, d * half : (d + 1) * half] * factor[d][:, part]
                for c in range(3):
                    grads[e, d, c, n, :, part] = value[c * modes : (c + 1) * modes].astype(
                        jnp.bfloat16
                    )
        value = jnp.dot(stacked, table_t[...], preferred_element_type=jnp.float32) * factor[2]
        for c in range(3):
            grads[e, 2, c, n] = value[c * modes : (c + 1) * modes].astype(jnp.bfloat16)

    def own_panel(e, carry):
        differentiate(t, e)
        for c in range(3):
            own = fields[t, e, c].astype(jnp.float32)
            for i in range(modes):
                wide[e, c * modes + i] = jnp.broadcast_to(
                    own[i : i + 1], (rows16, cube)
                ).astype(jnp.bfloat16)
        return carry

    lax.fori_loop(0, elements, own_panel, 0)
    totals[...] = jnp.zeros_like(totals)

    def arrive(e):
        for off in range(1, n_test):
            panel_copy(off, e).wait_recv()
            differentiate(lax.rem(t + n_test - off, n_test), e)
        for d in range(3):
            rhs[e, d] = jnp.concatenate([fields[n, e, d] for n in range(n_test)], axis=0).T

    def block(e, ib):
        total = jnp.zeros((block_modes * all_modes, all_modes), jnp.float32)
        for d in range(3):
            for h in range(2):
                part = slice(h * half, (h + 1) * half)
                g = [
                    grads[e, d, c, :, :, part].reshape(all_modes // rows16, rows16, half)
                    for c in range(3)
                ]
                pairs = []
                for i in range(block_modes):
                    row = ib * block_modes + i
                    f = [wide[e, c * modes + row, :, part][None] for c in range(3)]
                    summed = f[0] * g[0] + f[1] * g[1] + f[2] * g[2]
                    pairs.append(summed.reshape(all_modes, half))
                total = total + jnp.dot(
                    jnp.concatenate(pairs, axis=0),
                    rhs[e, d, part, :],
                    preferred_element_type=jnp.float32,
                )
        totals[ib] += total

    def loop(start, stop, work):
        def step(index, carry):
            work(index)
            return carry

        lax.fori_loop(start, stop, step, 0)

    def element(e):
        arrive(e)
        loop(0, blocks, lambda ib: block(e, ib))

    loop(0, elements - tail, element)
    loop(elements - tail, elements, arrive)

    def finish(ib):
        loop(elements - tail, elements, lambda e: block(e, ib))
        turned = totals[ib].T
        for b in range(n_elem):
            rows = turned[b * owned : (b + 1) * owned]
            outgoing[ib, b] = jnp.concatenate(
                [rows[:, q * lane_width : (q + 1) * lane_width] for q in range(parts)], axis=0
            ).astype(jnp.bfloat16)
        for off in range(1, n_elem):
            sum_copy(off, ib).start()

    loop(0, blocks, finish)

    def drain(e):
        for off in range(1, n_test):
            panel_copy(off, e).wait_send()

    loop(0, elements, drain)

    def collect(ib):
        result = outgoing[ib, me].astype(jnp.float32)
        for off in range(1, n_elem):
            sum_copy(off, ib).wait_recv()
            result = result + incoming[ib, off - 1].astype(jnp.float32)
        out_ref[ib] = result * final_scale
        for off in range(1, n_elem):
            sum_copy(off, ib).wait_send()

    loop(0, blocks, collect)


def split_tables(order_points):
    table, cube_weights = lobatto_tables(order_points)
    cube = order_points**3
    half = cube // 2
    table_rs = np.concatenate([table[:half, :half], table[:half, cube : cube + half]], axis=1)
    table_t = table[:, 2 * cube :]
    return table_rs, table_t, cube_weights


def body(mode_fields, elem_type, type_scales):
    n_test = lax.axis_size("test")
    n_elem = lax.axis_size("elem")
    cube = Q**3
    modes, _, points = mode_fields.shape
    elements = points // cube
    all_modes = modes * n_test
    owned = all_modes // n_elem
    blocks = modes // block_modes
    table_rs, table_t, cube_weights = split_tables(Q)
    final_scale = float(points * n_elem) ** (-0.5)
    lanes = block_modes * all_modes
    parts = lanes // lane_width
    rows = parts * owned
    vmem = pl.BlockSpec(memory_space=pltpu.VMEM)
    far = pl.BlockSpec(memory_space=pl.ANY)
    smem = pl.BlockSpec(memory_space=pltpu.SMEM)

    def call(*args):
        kernel(n_test, n_elem, elements, final_scale, *args)

    out = pl.pallas_call(
        call,
        out_shape=jax.ShapeDtypeStruct((blocks, rows, lane_width), jnp.float32),
        in_specs=[far, smem, smem, far, far, vmem],
        out_specs=vmem,
        scratch_shapes=[
            pltpu.VMEM(table_rs.shape, jnp.bfloat16),
            pltpu.VMEM(table_t.shape, jnp.bfloat16),
            pltpu.SemaphoreType.DMA((2,)),
            pltpu.VMEM((n_test, elements, 3, modes, cube), jnp.bfloat16),
            pltpu.VMEM((elements, 3, 3, n_test, modes, cube), jnp.bfloat16),
            pltpu.VMEM((elements, 3 * modes, rows16, cube), jnp.bfloat16),
            pltpu.VMEM((elements, 3, cube, all_modes), jnp.bfloat16),
            pltpu.VMEM((blocks, lanes, all_modes), jnp.float32),
            pltpu.VMEM((blocks, n_elem, rows, lane_width), jnp.bfloat16),
            pltpu.VMEM((blocks, n_elem - 1, rows, lane_width), jnp.bfloat16),
            pltpu.SemaphoreType.DMA((elements,)),
            pltpu.SemaphoreType.DMA((n_test - 1, elements)),
            pltpu.SemaphoreType.DMA((n_test - 1, elements)),
            pltpu.SemaphoreType.DMA((blocks, n_elem - 1)),
            pltpu.SemaphoreType.DMA((blocks, n_elem - 1)),
        ],
        compiler_params=pltpu.CompilerParams(
            collective_id=0, has_side_effects=True, vmem_limit_bytes=60 * 1024 * 2**10
        ),
    )(
        mode_fields.transpose(1, 0, 2),
        elem_type,
        type_scales,
        jnp.asarray(table_rs).astype(jnp.bfloat16),
        jnp.asarray(table_t).astype(jnp.bfloat16),
        jnp.asarray(cube_weights)[None, :],
    )
    return (
        out.reshape(blocks, parts, owned, lane_width // all_modes, all_modes)
        .transpose(0, 1, 3, 2, 4)
        .reshape(modes, owned, all_modes)
    )


def solution(mesh):
    placed = (P("test", None, "elem"), P("elem"), P())
    return jax.shard_map(
        body, mesh=mesh, in_specs=placed, out_specs=P("test", "elem", None), check_vma=False
    )
```

```python
import jax
import jax.numpy as jnp
import numpy as np
from jax import lax
from jax.experimental import pallas as pl
from jax.experimental.pallas import tpu as pltpu
from jax.sharding import PartitionSpec as P

Q = 8


block_modes = 8
many_modes = 16
rows16 = 16
lane_width = 128
tail_elements = 2


def legendre_top(points, degree):
    before = points * 0.0 + 1.0
    current = points
    for order in range(2, degree + 1):
        following = ((2 * order - 1) * points * current - (order - 1) * before) / order
        before = current
        current = following
    return (current, before)


def lobatto_tables(order_points):
    degree = order_points - 1
    lobatto_nodes = np.cos(np.pi * np.arange(degree + 1) / degree)
    for sweep in range(100):
        top, lower = legendre_top(lobatto_nodes, degree)
        lobatto_nodes = lobatto_nodes - (lobatto_nodes * top - lower) / ((degree + 1) * top)
    lobatto_nodes = lobatto_nodes[::-1].copy()
    lobatto_nodes[0] = -1.0
    lobatto_nodes[-1] = 1.0
    values, unused = legendre_top(lobatto_nodes, degree)
    weights = 2.0 / (degree * (degree + 1) * values**2)
    identity = np.eye(order_points)
    distance = lobatto_nodes[:, None] - lobatto_nodes[None, :]
    spacing = np.where(identity > 0, 1.0, distance)
    derivative = np.where(identity > 0, 0.0, values[:, None] / values[None, :] / spacing)
    corner = degree * (degree + 1) / 4.0
    ends = np.concatenate([[-corner], np.zeros(degree - 1), [corner]])
    derivative = derivative + identity * ends[None, :]
    square_eye = np.eye(order_points * order_points)
    along_r = np.kron(square_eye, derivative)
    along_s = np.kron(identity, np.kron(derivative, identity))
    along_t = np.kron(derivative, square_eye)
    table = np.concatenate([along_r.T, along_s.T, along_t.T], axis=1)
    cube_weights = np.kron(weights, np.kron(weights, weights))
    return (table.astype(np.float32), cube_weights.astype(np.float32))


def kernel(
    n_test, n_elem, elements, final_scale,
    x_ref, types, type_scales, far_rs, far_t, weights,
    out_ref,
    table_rs, table_t, table_sem, fields, grads, wide, rhs, totals, outgoing, incoming,
    local_sem, send_sem, recv_sem, send_sum, recv_sum,
):
    _, modes, points = x_ref.shape
    cube = points // elements
    all_modes = n_test * modes
    half = cube // 2
    owned = all_modes // n_elem
    blocks = modes // block_modes
    parts = block_modes * all_modes // lane_width
    tail = min(tail_elements, elements)
    many = many_modes if modes % many_modes == 0 else block_modes
    t = lax.axis_index("test")
    me = lax.axis_index("elem")

    def local_copy(e):
        return pltpu.make_async_copy(
            x_ref.at[:, :, pl.ds(e * cube, cube)], fields.at[t, e], local_sem.at[e]
        )

    def panel_copy(off, e):
        return pltpu.make_async_remote_copy(
            src_ref=fields.at[t, e],
            dst_ref=fields.at[t, e],
            send_sem=send_sem.at[off - 1, e],
            recv_sem=recv_sem.at[off - 1, e],
            device_id={"test": lax.rem(t + off, n_test)},
            device_id_type=pl.DeviceIdType.MESH,
        )

    def sum_copy(off, ib):
        return pltpu.make_async_remote_copy(
            src_ref=outgoing.at[ib, lax.rem(me + off, n_elem)],
            dst_ref=incoming.at[ib, off - 1],
            send_sem=send_sum.at[ib, off - 1],
            recv_sem=recv_sum.at[ib, off - 1],
            device_id={"elem": lax.rem(me + off, n_elem)},
            device_id_type=pl.DeviceIdType.MESH,
        )

    barrier = pltpu.get_barrier_semaphore()
    for off in range(1, n_test):
        pl.semaphore_signal(
            barrier, inc=1, device_id={"test": lax.rem(t + off, n_test)},
            device_id_type=pl.DeviceIdType.MESH,
        )
    for off in range(1, n_elem):
        pl.semaphore_signal(
            barrier, inc=1, device_id={"elem": lax.rem(me + off, n_elem)},
            device_id_type=pl.DeviceIdType.MESH,
        )
    for e in range(elements):
        local_copy(e).start()
    tables = [
        pltpu.make_async_copy(far_rs, table_rs, table_sem.at[0]),
        pltpu.make_async_copy(far_t, table_t, table_sem.at[1]),
    ]
    for copy in tables:
        copy.start()
    pl.semaphore_wait(barrier, n_test + n_elem - 2)

    for e in range(elements):
        local_copy(e).wait()
        for off in range(1, n_test):
            panel_copy(off, e).start()

    for copy in tables:
        copy.wait()

    def differentiate(n, e):
        kind = types[e]
        scale = [type_scales[kind, d] for d in range(3)]
        volume = jnp.full((1, cube), scale[0] * scale[1] * scale[2], jnp.float32)
        quadrature = weights[...] / volume
        factor = [quadrature * scale[d] for d in range(3)]
        stacked = jnp.concatenate([fields[n, e, c] for c in range(3)], axis=0)
        for h in range(2):
            part = slice(h * half, (h + 1) * half)
            derived = jnp.dot(
                stacked[:, part], table_rs[...], preferred_element_type=jnp.float32
            )
            for d in range(2):
                value = derived[:, d * half : (d + 1) * half] * factor[d][:, part]
                for c in range(3):
                    grads[e, d, c, n, :, part] = value[c * modes : (c + 1) * modes].astype(
                        jnp.bfloat16
                    )
        value = jnp.dot(stacked, table_t[...], preferred_element_type=jnp.float32) * factor[2]
        for c in range(3):
            grads[e, 2, c, n] = value[c * modes : (c + 1) * modes].astype(jnp.bfloat16)

    def own_panel(e, carry):
        differentiate(t, e)
        for c in range(3):
            own = fields[t, e, c].astype(jnp.float32)
            for i in range(modes):
                wide[e, c * modes + i] = jnp.broadcast_to(
                    own[i : i + 1], (rows16, cube)
                ).astype(jnp.bfloat16)
        return carry

    lax.fori_loop(0, elements, own_panel, 0)
    totals[...] = jnp.zeros_like(totals)

    def arrive(e):
        for off in range(1, n_test):
            panel_copy(off, e).wait_recv()
            differentiate(lax.rem(t + n_test - off, n_test), e)
        for d in range(3):
            rhs[e, d] = jnp.concatenate([fields[n, e, d] for n in range(n_test)], axis=0).T

    def block(e, step, count):
        total = jnp.zeros((count * all_modes, all_modes), jnp.float32)
        for d in range(3):
            for h in range(2):
                part = slice(h * half, (h + 1) * half)
                g = [
                    grads[e, d, c, :, :, part].reshape(all_modes // rows16, rows16, half)
                    for c in range(3)
                ]
                pairs = []
                for i in range(count):
                    row = step * count + i
                    f = [wide[e, c * modes + row, :, part][None] for c in range(3)]
                    summed = f[0] * g[0] + f[1] * g[1] + f[2] * g[2]
                    pairs.append(summed.reshape(all_modes, half))
                total = total + jnp.dot(
                    jnp.concatenate(pairs, axis=0),
                    rhs[e, d, part, :],
                    preferred_element_type=jnp.float32,
                )
        held = count // block_modes
        lanes = block_modes * all_modes
        for b in range(held):
            totals[step * held + b] += total[b * lanes : (b + 1) * lanes]

    def loop(start, stop, work):
        def step(index, carry):
            work(index)
            return carry

        lax.fori_loop(start, stop, step, 0)

    def element(e):
        arrive(e)
        loop(0, modes // many, lambda step: block(e, step, many))

    loop(0, elements - tail, element)
    loop(elements - tail, elements, arrive)

    def finish(ib):
        loop(elements - tail, elements, lambda e: block(e, ib, block_modes))
        turned = totals[ib].T
        for b in range(n_elem):
            rows = turned[b * owned : (b + 1) * owned]
            outgoing[ib, b] = jnp.concatenate(
                [rows[:, q * lane_width : (q + 1) * lane_width] for q in range(parts)], axis=0
            ).astype(jnp.bfloat16)
        for off in range(1, n_elem):
            sum_copy(off, ib).start()

    loop(0, blocks, finish)

    def drain(e):
        for off in range(1, n_test):
            panel_copy(off, e).wait_send()

    loop(0, elements, drain)

    def collect(ib):
        result = outgoing[ib, me].astype(jnp.float32)
        for off in range(1, n_elem):
            sum_copy(off, ib).wait_recv()
            result = result + incoming[ib, off - 1].astype(jnp.float32)
        out_ref[ib] = result * final_scale
        for off in range(1, n_elem):
            sum_copy(off, ib).wait_send()

    loop(0, blocks, collect)


def split_tables(order_points):
    table, cube_weights = lobatto_tables(order_points)
    cube = order_points**3
    half = cube // 2
    table_rs = np.concatenate([table[:half, :half], table[:half, cube : cube + half]], axis=1)
    table_t = table[:, 2 * cube :]
    return table_rs, table_t, cube_weights


def body(mode_fields, elem_type, type_scales):
    n_test = lax.axis_size("test")
    n_elem = lax.axis_size("elem")
    cube = Q**3
    modes, _, points = mode_fields.shape
    elements = points // cube
    all_modes = modes * n_test
    owned = all_modes // n_elem
    blocks = modes // block_modes
    table_rs, table_t, cube_weights = split_tables(Q)
    final_scale = float(points * n_elem) ** (-0.5)
    lanes = block_modes * all_modes
    parts = lanes // lane_width
    rows = parts * owned
    vmem = pl.BlockSpec(memory_space=pltpu.VMEM)
    far = pl.BlockSpec(memory_space=pl.ANY)
    smem = pl.BlockSpec(memory_space=pltpu.SMEM)

    def call(*args):
        kernel(n_test, n_elem, elements, final_scale, *args)

    out = pl.pallas_call(
        call,
        out_shape=jax.ShapeDtypeStruct((blocks, rows, lane_width), jnp.float32),
        in_specs=[far, smem, smem, far, far, vmem],
        out_specs=vmem,
        scratch_shapes=[
            pltpu.VMEM(table_rs.shape, jnp.bfloat16),
            pltpu.VMEM(table_t.shape, jnp.bfloat16),
            pltpu.SemaphoreType.DMA((2,)),
            pltpu.VMEM((n_test, elements, 3, modes, cube), jnp.bfloat16),
            pltpu.VMEM((elements, 3, 3, n_test, modes, cube), jnp.bfloat16),
            pltpu.VMEM((elements, 3 * modes, rows16, cube), jnp.bfloat16),
            pltpu.VMEM((elements, 3, cube, all_modes), jnp.bfloat16),
            pltpu.VMEM((blocks, lanes, all_modes), jnp.float32),
            pltpu.VMEM((blocks, n_elem, rows, lane_width), jnp.bfloat16),
            pltpu.VMEM((blocks, n_elem - 1, rows, lane_width), jnp.bfloat16),
            pltpu.SemaphoreType.DMA((elements,)),
            pltpu.SemaphoreType.DMA((n_test - 1, elements)),
            pltpu.SemaphoreType.DMA((n_test - 1, elements)),
            pltpu.SemaphoreType.DMA((blocks, n_elem - 1)),
            pltpu.SemaphoreType.DMA((blocks, n_elem - 1)),
        ],
        compiler_params=pltpu.CompilerParams(
            collective_id=0, has_side_effects=True, vmem_limit_bytes=60 * 1024 * 2**10
        ),
    )(
        mode_fields.transpose(1, 0, 2),
        elem_type,
        type_scales,
        jnp.asarray(table_rs).astype(jnp.bfloat16),
        jnp.asarray(table_t).astype(jnp.bfloat16),
        jnp.asarray(cube_weights)[None, :],
    )
    return (
        out.reshape(blocks, parts, owned, lane_width // all_modes, all_modes)
        .transpose(0, 1, 3, 2, 4)
        .reshape(modes, owned, all_modes)
    )


def solution(mesh):
    placed = (P("test", None, "elem"), P("elem"), P())
    return jax.shard_map(
        body, mesh=mesh, in_specs=placed, out_specs=P("test", "elem", None), check_vma=False
    )
```
